32 devices in a mesh: seq: 8 (over y, x, core), head: 4 (over z).
Axes of the slice: x: 2, y: 2, z: 4, core: 2. Of those that a mesh axis runs over, the one named last changes fastest.
Arguments:
- latent: bfloat16 [1024, 1024], P('seq'), may hold values from -15 to 15
- probe: bfloat16 [1024, 1024], P('seq'), may hold values from -6 to 6
- time_embed: float32 [1024], replicated, may hold values from -6 to 6
- gain_attn: float32 [1024], replicated, may hold values from 0.1 to 1.9
- w_query: bfloat16 [1024, 1024], P(None, 'head'), may hold values from -0.625 to 0.625
- w_key: bfloat16 [1024, 1024], P(None, 'head'), may hold values from -11 to 11
- w_value: bfloat16 [1024, 1024], P(None, 'head'), may hold values from -0.1875 to 0.1875
- w_out: bfloat16 [1024, 1024], P('head'), may hold values from -0.1875 to 0.1875
- gain_mlp: float32 [1024], replicated, may hold values from 0.1 to 1.9
- w_in: bfloat16 [1024, 4096], P(None, 'head'), may hold values from -0.1875 to 0.1875
- w_down: bfloat16 [4096, 1024], P('head'), may hold values from -0.09375 to 0.09375
Outputs:
- latent_end: float32 [1024, 1024], P('seq')
- frame_trace: float32 [1024], P('seq')
- frame_logp: float32 [1024], P('seq')
- mean_logp: float32 [], replicated
The draws below stay inside these ranges and needn't reach their ends.
All inputs are finite; a program needn't handle non-finite values.
Results may differ from the reference program's by a relative error of at most 0.03.
The reference program's roundings to bfloat16 on the way count: a program that leaves them out, or rounds other values in their place, can miss the bound.
Values may be sent and summed in bfloat16 or wider, within the bound.
A program may use at most 64 MiB of HBM per device.

```python
import math
import jax
import jax.numpy as jnp
from jax import lax

D = 1024
HEADS = 16
HEAD_DIM = 64
FF = 4096
STEPS = 2
FRAMES = 1024


def weight_pair(key):
    base = jax.random.fold_in(key, 11)
    first, second = jax.random.split(base, 2)
    query_weight = jnp.clip(jax.random.normal(first, (D, D), jnp.float32), -5.0, 5.0) * D ** (-0.5)
    noise = jnp.clip(jax.random.normal(second, (D, D), jnp.float32), -5.0, 5.0) * D ** (-0.5)
    key_weight = 3.0 * noise
    return (query_weight, key_weight)


def draw_w_query(key, part):
    return weight_pair(key)[0].astype(jnp.bfloat16)


def draw_w_key(key, part):
    return weight_pair(key)[1].astype(jnp.bfloat16)


def draw_latent(key, part):
    base = jax.random.fold_in(key, 23)
    position = jnp.arange(FRAMES, dtype=jnp.float32) / max(FRAMES - 1, 1)
    entries = jnp.clip(jax.random.normal(base, (FRAMES, D), jnp.float32), -5.0, 5.0)
    ramp = 1.0 + 2.0 * position
    return (entries * ramp[:, None]).astype(jnp.bfloat16)


def steps_of(key, extent, shards, low, high):
    factor_of, own = 1.0, jax.random.fold_in(key, 6)
    for dim, blocks in shards:
        heights = jnp.exp(jax.random.uniform(jax.random.fold_in(own, dim), (blocks,), jnp.float32, low / len(shards), high / len(shards)))
        factor_of = factor_of * jnp.repeat(heights, extent[dim] // blocks).reshape([-1 if axis == dim else 1 for axis in range(len(extent))])
    return factor_of


def normal_values(stream_key, extent, deviation, most, shards=(), held_as=jnp.bfloat16):
    array = jax.random.normal(stream_key, extent, jnp.float32) * deviation
    if len(shards) > 0:
        array = steps_of(stream_key, extent, shards, -0.22, 0.18) * array
    return jnp.clip(array, min=-most, max=most).astype(held_as)


def setup_inputs(seed: int = 0) -> dict:
    key_of = jax.random.split(jax.random.key(seed), 12)
    latent = draw_latent(jax.random.fold_in(key_of[11], 71), 0)
    probe = normal_values(key_of[1], (FRAMES, D), 1.0, 6.0, ((0, 8),))
    time_embed = normal_values(key_of[2], (D,), 1.0, 6.0, (), jnp.float32)
    gain_attn = jnp.clip(1.0 + 0.18 * jax.random.normal(key_of[3], (D,), jnp.float32), 0.1, 1.9)
    w_query = draw_w_query(jax.random.fold_in(key_of[11], 71), 0)
    w_key = draw_w_key(jax.random.fold_in(key_of[11], 71), 0)
    w_value = normal_values(key_of[6], (D, D), D ** -0.5, 0.1875, ((1, 4),))
    w_out = normal_values(key_of[7], (D, D), D ** -0.5, 0.1875, ((0, 4),))
    gain_mlp = jnp.clip(1.0 + 0.18 * jax.random.normal(key_of[8], (D,), jnp.float32), 0.1, 1.9)
    w_in = normal_values(key_of[9], (D, FF), D ** -0.5, 0.1875, ((1, 4),))
    w_down = normal_values(key_of[10], (FF, D), FF ** -0.5, 0.09375, ((0, 4),))
    return dict(latent=latent, probe=probe, time_embed=time_embed, gain_attn=gain_attn, w_query=w_query, w_key=w_key, w_value=w_value, w_out=w_out, gain_mlp=gain_mlp, w_in=w_in, w_down=w_down)


EPSILON = 1e-05
GELU_COEF = 0.044715
ROOT_TWO_PI = math.sqrt(2.0 / math.pi)

def norm_pair(values, tangent, norm_gain):
    meansq = lax.optimization_barrier(jnp.mean(values * values, axis=-1, keepdims=True)) + EPSILON
    inverse = lax.rsqrt(meansq)
    inner_mean = lax.optimization_barrier(jnp.mean(values * tangent, axis=-1, keepdims=True))
    primal = values * inverse * norm_gain
    derived = (tangent * inverse - values * inverse ** 3 * inner_mean) * norm_gain
    return (primal.astype(jnp.bfloat16), derived.astype(jnp.bfloat16))

def gelu_pair(pre_act, tangent):
    cubic_arg = pre_act + GELU_COEF * pre_act ** 3
    tanh_value = jnp.tanh(ROOT_TWO_PI * cubic_arg)
    output = 0.5 * pre_act * (1.0 + tanh_value)
    slope_value = 0.5 * (1.0 + tanh_value) + 0.5 * pre_act * (1.0 - tanh_value * tanh_value) * ROOT_TWO_PI * (1.0 + 3.0 * GELU_COEF * pre_act * pre_act)
    return (output.astype(jnp.bfloat16), (slope_value * tangent).astype(jnp.bfloat16))

def attention(queries, query_tang, keys, vals, key_tang, val_tang):
    scale = HEAD_DIM ** (-0.5)

    def heads_of(matrix):
        return matrix.astype(jnp.float32).reshape(FRAMES, HEADS, HEAD_DIM)
    keys_all = heads_of(keys)
    vals_all = heads_of(vals)
    key_tang_all = heads_of(key_tang)
    val_tang_all = heads_of(val_tang)
    block = math.gcd(FRAMES, 512)

    def one_block(pair):
        block_queries, block_tang = pair
        scores = jnp.einsum('bhd,shd->hbs', block_queries, keys_all) * scale
        score_tang = (jnp.einsum('bhd,shd->hbs', block_tang, keys_all) + jnp.einsum('bhd,shd->hbs', block_queries, key_tang_all)) * scale
        row_top = lax.optimization_barrier(jnp.max(scores, axis=-1, keepdims=True))
        weights = jnp.exp(scores - row_top)
        total = lax.optimization_barrier(jnp.sum(weights, axis=-1))
        weighted = weights * score_tang
        carried = lax.optimization_barrier(jnp.sum(weighted, axis=-1))
        rounded = lax.optimization_barrier(weights.astype(jnp.bfloat16)).astype(jnp.float32)
        rounded_tang = lax.optimization_barrier(weighted.astype(jnp.bfloat16)).astype(jnp.float32)
        acc_primal = jnp.einsum('hbs,shd->bhd', rounded, vals_all)
        acc_tang = jnp.einsum('hbs,shd->bhd', rounded_tang, vals_all) + jnp.einsum('hbs,shd->bhd', rounded, val_tang_all)
        total_t = jnp.transpose(total)[:, :, None]
        carried_t = jnp.transpose(carried)[:, :, None]
        primal = acc_primal / total_t
        tangent = acc_tang / total_t - carried_t / total_t * primal
        return (primal.astype(jnp.bfloat16), tangent.astype(jnp.bfloat16))
    query_blocks = heads_of(queries).reshape(FRAMES // block, block, HEADS, HEAD_DIM)
    tang_blocks = heads_of(query_tang).reshape(FRAMES // block, block, HEADS, HEAD_DIM)
    head_out, head_tang = lax.map(one_block, (query_blocks, tang_blocks))
    return (head_out.reshape(FRAMES, D), head_tang.reshape(FRAMES, D))

def vector_field(inputs, direction, gain_attn, w_query, w_key, w_value, w_out, gain_mlp, w_in, w_down):
    normed, normed_tang = norm_pair(inputs, direction, gain_attn)

    def project(weight):
        primal = jnp.dot(normed, weight, preferred_element_type=jnp.float32).astype(jnp.bfloat16)
        tangent = jnp.dot(normed_tang, weight, preferred_element_type=jnp.float32).astype(jnp.bfloat16)
        return (primal, tangent)
    queries, query_tang = project(w_query)
    keys, key_tang = project(w_key)
    vals, val_tang = project(w_value)
    head_out, head_tang = attention(queries, query_tang, keys, vals, key_tang, val_tang)
    attn = jnp.dot(head_out, w_out, preferred_element_type=jnp.float32)
    attn_tang = jnp.dot(head_tang, w_out, preferred_element_type=jnp.float32)
    middle = inputs + attn
    middle_tang = direction + attn_tang
    normed_mlp, normed_mlp_tang = norm_pair(middle, middle_tang, gain_mlp)
    pre_act = jnp.dot(normed_mlp, w_in, preferred_element_type=jnp.float32)
    pre_tang = jnp.dot(normed_mlp_tang, w_in, preferred_element_type=jnp.float32)
    activ, activ_tang = gelu_pair(pre_act, pre_tang)
    mlp_out = jnp.dot(activ, w_down, preferred_element_type=jnp.float32)
    mlp_tang = jnp.dot(activ_tang, w_down, preferred_element_type=jnp.float32)
    return (attn + mlp_out, attn_tang + mlp_tang)

def reference(latent, probe, time_embed, gain_attn, w_query, w_key, w_value, w_out, gain_mlp, w_in, w_down):
    state = latent.astype(jnp.float32)
    direction = probe.astype(jnp.float32)
    trace = jnp.zeros((FRAMES,), jnp.float32)
    for euler_step in range(STEPS):
        inputs = state + euler_step / STEPS * time_embed
        field, field_tang = vector_field(inputs, direction, gain_attn, w_query, w_key, w_value, w_out, gain_mlp, w_in, w_down)
        trace = trace + lax.optimization_barrier(jnp.sum(direction * field_tang, axis=-1)) / (STEPS * D)
        state = state + field / STEPS
    frame_logp = trace - 0.5 * lax.optimization_barrier(jnp.sum(state * state, axis=-1)) / D - 0.5 * math.log(2.0 * math.pi)
    mean_logp = jnp.mean(frame_logp)
    return (state, trace, frame_logp, mean_logp)
```

```python
import functools
import math

import jax
import jax.numpy as jnp
from jax import lax
from jax.experimental import pallas as pl
from jax.experimental.pallas import tpu as pltpu
from jax.sharding import PartitionSpec as P

HEAD_DIM = 64
STEPS = 2
EPSILON = 1e-05
GELU_COEF = 0.044715
ROOT_TWO_PI = math.sqrt(2.0 / math.pi)
LANES = 128
CHUNKS = 2
BF16 = jnp.bfloat16
F32 = jnp.float32


def norm_scale(values):
    return lax.rsqrt(jnp.mean(values * values, axis=-1, keepdims=True) + EPSILON)


def norm_tangent(values, tangent, inverse, norm_gain):
    inner_mean = jnp.mean(values * tangent, axis=-1, keepdims=True)
    cubed = inverse * inverse * inverse
    return ((tangent * inverse - values * (cubed * inner_mean)) * norm_gain).astype(BF16)


def gelu_slope(pre_act):
    square = pre_act * pre_act
    tanh_value = jnp.tanh(ROOT_TWO_PI * pre_act * (1.0 + GELU_COEF * square))
    half = 0.5 * (1.0 + tanh_value)
    slope_value = half + 0.5 * pre_act * (1.0 - tanh_value * tanh_value) * (
        ROOT_TWO_PI * (1.0 + 3.0 * GELU_COEF * square)
    )
    return ((pre_act * half).astype(BF16), slope_value)


def dot(a, b):
    return jnp.dot(a, b, preferred_element_type=F32)


def dot_t(a, b):
    return lax.dot_general(a, b, (((1,), (1,)), ((), ())), preferred_element_type=F32)


def flow_kernel(
    n,
    m,
    latent,
    probe,
    time_embed,
    gain_attn,
    gain_mlp,
    w_query,
    w_key,
    w_value,
    w_out,
    w_in,
    w_down,
    latent_end,
    stats_out,
    mean_out,
    wqkv,
    wout,
    win,
    wdown,
    normed,
    qbuf,
    kbuf,
    vbuf,
    headall,
    inbuf,
    probe_down,
    weightbuf,
    primbuf,
    totalbuf,
    midbuf,
    slopebuf,
    partial,
    rssend,
    rsrecv,
    state,
    delta,
    tracebuf,
    sumbuf,
    lsem,
    wsend,
    wrecv,
    gsend,
    grecv,
    kvsend,
    kvrecv,
    zsend,
    zrecv,
    tsend,
    trecv,
    msend,
    mrecv,
):
    s = lax.axis_index("seq")
    z = lax.axis_index("head")
    rows, width = latent.shape
    part = rows // m
    piece = width // CHUNKS
    cols = w_query.shape[1]
    pairs = cols // LANES
    frames = rows * n
    near = n == 8

    def flip(bit):
        return s + bit - 2 * bit * lax.rem(s // bit, 2)

    def zpeer(d):
        return lax.rem(z + d, m)

    def zfrom(d):
        return lax.rem(z + m - d, m)

    def remote(src, dst, send, recv, target_s, target_z):
        return pltpu.make_async_remote_copy(
            src_ref=src,
            dst_ref=dst,
            send_sem=send,
            recv_sem=recv,
            device_id=(target_s, target_z),
            device_id_type=pl.DeviceIdType.MESH,
        )

    scope = [None]

    def S(name):
        if scope[0] is not None:
            scope[0].__exit__(None, None, None)
        scope[0] = None
        if name is not None:
            scope[0] = jax.named_scope(name)
            scope[0].__enter__()

    S("start")
    loads = [
        pltpu.make_async_copy(w_query, wqkv.at[:, pl.ds(0, cols)], lsem.at[0]),
        pltpu.make_async_copy(w_key, wqkv.at[:, pl.ds(cols, cols)], lsem.at[1]),
        pltpu.make_async_copy(w_value, wqkv.at[:, pl.ds(2 * cols, cols)], lsem.at[2]),
        pltpu.make_async_copy(w_out, wout.at[z], lsem.at[3]),
        pltpu.make_async_copy(w_in, win, lsem.at[4]),
        pltpu.make_async_copy(w_down, wdown, lsem.at[5]),
    ]
    for index in (3, 1, 2, 0, 5, 4):
        loads[index].start()

    barrier = pltpu.get_barrier_semaphore()

    def everyone():
        for a in range(n):
            for b in range(m):
                if a or b:
                    yield a * m + b, lax.rem(s + a, n), lax.rem(z + b, m)

    for _, target_s, target_z in everyone():
        pl.semaphore_signal(
            barrier, inc=1, device_id=(target_s, target_z), device_id_type=pl.DeviceIdType.MESH
        )

    own_rows = pl.ds(pl.multiple_of(z * part, part), part)
    direction = probe[...].astype(F32)

    def norm_inputs(values):
        inverse = norm_scale(values)
        normed[:rows, :] = (values * inverse * gain_attn[...]).astype(BF16)
        return inverse

    def norm_inputs_tangent(values, inverse):
        normed[rows:, :] = norm_tangent(
            values, probe[...].astype(F32), inverse, gain_attn[...]
        )

    first_values = latent[...].astype(F32)
    inbuf[...] = first_values
    inverse = norm_inputs(first_values)
    norm_inputs_tangent(first_values, inverse)
    state[...] = latent[own_rows, :].astype(F32)

    S("barrier")
    pl.semaphore_wait(barrier, n * m - 1)

    partner = flip(1)
    xn, yn = flip(2), flip(4)
    dn = yn + 2 - 4 * lax.rem(yn // 2, 2)

    def exchange(view, send_sem, recv_sem):
        sends = []

        def give(which, slot, target, at):
            copy = remote(
                view(which, slot),
                view(which, slot),
                send_sem(len(sends)),
                recv_sem(which, at),
                target,
                z,
            )
            copy.start()
            sends.append(copy)

        def got(which, slot, at):
            pltpu.make_async_copy(
                view(which, slot), view(which, slot), recv_sem(which, at)
            ).wait()

        def own(which):
            if near:
                first, second = ((xn, 2), (yn, 4)) if which == 0 else ((yn, 4), (xn, 2))
                give(which, s, *first)
                give(which, s, *second)
                give(which, s, partner, 1)
            else:
                for d in range(1, n):
                    give(which, s, lax.rem(s + d, n), d)

        def relay():
            if near:
                got(0, xn, 2)
                give(0, xn, yn, 6)
                got(1, yn, 4)
                give(1, yn, xn, 6)
                give(0, xn, partner, 3)
                give(1, yn, partner, 5)

        def rest():
            if near:
                got(0, yn, 4)
                give(0, yn, partner, 5)
                got(1, xn, 2)
                give(1, xn, partner, 3)
                got(0, dn, 6)
                give(0, dn, partner, 7)
                got(1, dn, 6)
                give(1, dn, partner, 7)

        def finish():
            if near:
                slots = ((s, 1), (xn, 3), (yn, 5), (dn, 7))
                for which in range(2):
                    for slot, at in slots:
                        got(which, slot + 1 - 2 * lax.rem(slot, 2), at)
            else:
                for which in range(2):
                    for d in range(1, n):
                        got(which, lax.rem(s + n - d, n), d)

        def drain():
            for copy in sends:
                copy.wait_send()

        return own, relay, rest, finish, drain

    def kv_exchange(k, t, p):
        bufs = (kbuf, vbuf)
        return exchange(
            lambda which, slot: bufs[which].at[k, t, p, slot],
            lambda index: kvsend.at[k, t, p, index],
            lambda which, at: kvrecv.at[k, t, p, which, at],
        )

    block = cols // n if near else cols
    strip = block // 2
    loads[3].wait()

    def block_at(slot):
        if near:
            return pl.ds(pl.multiple_of(slot * block, block), block)
        return pl.ds(0, cols)

    def strip_at(which, slot):
        return pl.ds(pl.multiple_of(slot * block + which * strip, strip), strip)

    fetch_order = [1, m - 1] + list(range(2, m - 1))
    fetches = {}
    for d in fetch_order:
        fetches[d] = remote(
            wout.at[z, block_at(s)],
            wout.at[z, block_at(s)],
            wsend.at[d],
            wrecv.at[d],
            s,
            zpeer(d),
        )
        fetches[d].start()

    def shard_exchange(d):
        return exchange(
            lambda which, slot: wout.at[zfrom(d), strip_at(which, slot)],
            lambda index: gsend.at[d, index],
            lambda which, at: grecv.at[d, which, at],
        )

    shards = {d: shard_exchange(d) for d in fetch_order} if near else {}

    def shard_own(d):
        fetches[d].wait_recv()
        if near:
            shards[d][0](0)
            shards[d][0](1)

    def z_start(k, phase, src_of, dst):
        copies = []
        for d in range(m - 1, 0, -1):
            copy = remote(
                src_of(zpeer(d)), dst, zsend.at[k, phase, d], zrecv.at[k, phase, d], s, zpeer(d)
            )
            copy.start()
            copies.append(copy)
        return copies

    def z_wait(copies):
        for copy in copies:
            copy.wait_send()
            copy.wait_recv()

    lane = lax.broadcasted_iota(jnp.int32, (1, LANES), 1)
    first = (lane // HEAD_DIM) == 0
    scale = HEAD_DIM ** (-0.5)

    def project(k, which, t):
        if k == 0 and t == 0:
            loads[which].wait()
        weight = wqkv[:, which * cols : (which + 1) * cols]
        return dot(normed[t * rows : (t + 1) * rows, :], weight).astype(BF16)

    def keep_pairs(ref, k, t, value):
        for p in range(pairs):
            ref[k, t, p, s] = value[:, p * LANES : (p + 1) * LANES]

    def two_heads(value):
        zero = jnp.zeros_like(value)
        return jnp.concatenate(
            [jnp.where(first, value, zero), jnp.where(first, zero, value)], axis=0
        )

    def join_heads(value):
        return jnp.where(first, value[:rows], value[rows:]).astype(BF16)

    def attention(k, p):
        keys = kbuf[k, 0, p].reshape(frames, LANES)
        vals = vbuf[k, 0, p].reshape(frames, LANES)
        scores = dot_t(two_heads(qbuf[0, p]), keys) * scale
        weights = jnp.exp(scores - jnp.max(scores, axis=-1, keepdims=True))
        total = jnp.sum(weights, axis=-1, keepdims=True)
        weightbuf[p] = weights
        prim = dot(weights.astype(BF16), vals) / total
        primbuf[p] = prim
        totalbuf[p] = jnp.broadcast_to(total, (2 * rows, LANES))
        headall[k, 0, p, z] = join_heads(prim)

    def attention_tangent(k, p):
        both_keys = jnp.concatenate(
            [kbuf[k, 0, p].reshape(frames, LANES), kbuf[k, 1, p].reshape(frames, LANES)], axis=1
        )
        vals = vbuf[k, 0, p].reshape(frames, LANES)
        val_tang = vbuf[k, 1, p].reshape(frames, LANES)
        both = jnp.concatenate([two_heads(qbuf[1, p]), two_heads(qbuf[0, p])], axis=1)
        score_tang = dot_t(both, both_keys) * scale
        weights = weightbuf[p]
        weighted = weights * score_tang
        carried = jnp.sum(weighted, axis=-1, keepdims=True)
        mixed = dot(weighted.astype(BF16), vals) + dot(weights.astype(BF16), val_tang)
        total = totalbuf[p]
        tang = mixed / total - (carried / total) * primbuf[p]
        headall[k, 1, p, z] = join_heads(tang)

    def heads_start(k, t, p):
        return z_start(k, t * pairs + p, lambda j: headall.at[k, t, p, z], headall.at[k, t, p, z])

    def out_project(k, t):
        heads = [headall[k, t, p, j] for j in range(m) for p in range(pairs)]
        return dot(jnp.concatenate(heads, axis=1), wout[...].reshape(m * cols, width))

    def mlp(k):
        attn = out_project(k, 0)
        mid = inbuf[...] + attn
        midbuf[...] = mid
        scaled = (mid * norm_scale(mid) * gain_mlp[...]).astype(BF16)
        if k == 0:
            loads[4].wait()
        act, slope = gelu_slope(dot(scaled, win[...]))
        slopebuf[...] = slope
        copies = []
        for c in range(CHUNKS):
            at = slice(c * piece, (c + 1) * piece)
            terms = dot(act, wdown[:, at])
            rssend[k, c] = terms.astype(BF16).reshape(m, part, piece)
            copies.append(
                z_start(
                    k,
                    2 * pairs + c,
                    lambda j: rssend.at[k, c, j],
                    rsrecv.at[k, c, z],
                )
            )
            partial[:, at] = attn[:, at] + terms
        return copies

    def mlp_tangent(k):
        attn_tang = out_project(k, 1)
        probing = probe[...].astype(F32)
        mid = midbuf[...]
        tangent = norm_tangent(mid, probing + attn_tang, norm_scale(mid), gain_mlp[...])
        act_tang = (slopebuf[...] * dot(tangent, win[...])).astype(BF16)
        return jnp.sum(probing * attn_tang, axis=-1, keepdims=True) / m + jnp.sum(
            act_tang.astype(F32) * probe_down[...], axis=-1, keepdims=True
        )

    trace = None
    tangent_heads = None
    all_exchanges = []

    for k in range(STEPS):
        last = k == STEPS - 1
        prims = [kv_exchange(k, 0, p) for p in range(pairs)]
        tangs = [kv_exchange(k, 1, p) for p in range(pairs)]
        all_exchanges += prims + tangs

        S(f"projk_{k}")
        keep_pairs(kbuf, k, 0, project(k, 1, 0))
        prims[0][0](0)
        S(f"projv_{k}")
        keep_pairs(vbuf, k, 0, project(k, 2, 0))
        prims[0][0](1)
        for p in range(1, pairs):
            prims[p][0](0)
            prims[p][0](1)
        if k > 0:
            S(f"tattn_{k-1}b")
            tangent_heads = [heads_start(k - 1, 1, p) for p in range(pairs)]
            norm_inputs_tangent(inbuf[...], inverse)
        S(f"projq_{k}")
        query = project(k, 0, 0)
        for p in range(pairs):
            qbuf[0, p] = query[:, p * LANES : (p + 1) * LANES]
        S(f"projt_{k}")
        keep_pairs(kbuf, k, 1, project(k, 1, 1))
        keep_pairs(vbuf, k, 1, project(k, 2, 1))
        S(f"relay0_{k}")
        prims[0][1]()
        S(f"projt2_{k}")
        query = project(k, 0, 1)
        for p in range(pairs):
            qbuf[1, p] = query[:, p * LANES : (p + 1) * LANES]
        S(f"relay1_{k}")
        for p in range(1, pairs):
            prims[p][1]()
        if k == 0:
            S(f"shard0_{k}")
            shard_own(fetch_order[0])
        else:
            for p in range(pairs):
                tangs[p][0](0)
                tangs[p][0](1)
        S(f"rest0_{k}")
        prims[0][2]()
        S(f"finish0_{k}")
        prims[0][3]()

        head_copies = []
        for p in range(pairs):
            if p > 0:
                S(f"rest1_{k}")
                prims[p][2]()
                prims[p][3]()
            S(f"attn_{k}_{p}")
            attention(k, p)
            head_copies.append(heads_start(k, 0, p))
            if k == 0 and p == 0:
                S(f"shard1_{k}")
                for d in fetch_order[1:]:
                    shard_own(d)

        if k == 0:
            S("probe_down")
            loads[5].wait()
            probe_down[...] = dot_t(probe[...], wdown[...])
            S("shard_relay")
            for d in shards:
                shards[d][1]()
            for p in range(pairs):
                tangs[p][0](0)
                tangs[p][0](1)
            S("shard_rest")
            for d in shards:
                shards[d][2]()
            for d in shards:
                shards[d][3]()
        else:
            for p in range(pairs):
                S(f"trelay_{k}_{p}")
                tangs[p][1]()
            for p in range(pairs):
                S(f"trest_{k}_{p}")
                tangs[p][2]()
                tangs[p][3]()
                S(f"tattn_{k}_{p}")
                attention_tangent(k, p)
                last_heads = heads_start(k, 1, p)
                later_heads = [last_heads] if p == 0 else later_heads + [last_heads]
            S(f"theads_{k-1}")
            for copies in tangent_heads:
                z_wait(copies)
            S(f"tmlp_{k-1}")
            trace = mlp_tangent(k - 1)
            tangent_heads = later_heads

        S(f"heads_{k}")
        for copies in head_copies:
            z_wait(copies)
        S(f"mlp_{k}")
        rs_copies = mlp(k)

        if not last:
            for p in range(pairs):
                S(f"trelay_{k}_{p}")
                tangs[p][1]()
            for p in range(pairs):
                S(f"trest_{k}_{p}")
                tangs[p][2]()
                tangs[p][3]()
                S(f"tattn_{k}_{p}")
                attention_tangent(k, p)
        else:
            S(f"theads_{k}")
            for copies in tangent_heads:
                z_wait(copies)
            S(f"tmlp_{k}")
            trace = trace + mlp_tangent(k)
            column = trace / (STEPS * width)
            trace_sum = jnp.sum(column, axis=0, keepdims=True)
            tracebuf[z] = jnp.transpose(jnp.broadcast_to(column, (rows, LANES)))[:8, :]
            trace_copies = []
            for d in range(1, m):
                copy = remote(
                    tracebuf.at[z], tracebuf.at[z], tsend.at[d], trecv.at[d], s, zpeer(d)
                )
                copy.start()
                trace_copies.append(copy)

        delta_copies = []
        squares = jnp.zeros((1, 1), F32)
        for c in range(CHUNKS):
            at = slice(c * piece, (c + 1) * piece)
            S(f"rswait_{k}_{c}")
            z_wait(rs_copies[c])
            S(f"field_{k}_{c}")
            field = partial[own_rows, at]
            for d in range(1, m):
                field = field + rsrecv[k, c, zfrom(d)].astype(F32)
            new_state = state[:, at] + field / STEPS
            state[:, at] = new_state
            delta[k, c, z] = (new_state - latent[own_rows, at].astype(F32)).astype(BF16)
            delta_copies.append(
                z_start(
                    k,
                    2 * pairs + CHUNKS + c,
                    lambda j: delta.at[k, c, z],
                    delta.at[k, c, z],
                )
            )
            if last:
                by_row = jnp.sum(new_state * new_state, axis=-1, keepdims=True)
                squares = squares + jnp.sum(by_row, axis=0, keepdims=True)
        if last:
            S("share")
            place = s * m + z
            sumbuf[place] = jnp.broadcast_to(trace_sum - 0.5 * squares / width, (1, LANES))
            mean_copies = []
            for index, target_s, target_z in everyone():
                copy = remote(
                    sumbuf.at[place],
                    sumbuf.at[place],
                    msend.at[index],
                    mrecv.at[index],
                    target_s,
                    target_z,
                )
                copy.start()
                mean_copies.append(copy)
            z_wait(trace_copies)
            trace_row = jnp.sum(tracebuf[...], axis=0)

        norm_sum = None
        for c in range(CHUNKS):
            at = slice(c * piece, (c + 1) * piece)
            S(f"deltawait_{k}_{c}")
            z_wait(delta_copies[c])
            S(f"norm_{k}_{c}")
            following = latent[:, at].astype(F32) + delta[k, c].reshape(rows, piece).astype(F32)
            if last:
                latent_end[:, at] = following
                norm_part = jnp.sum(following * following, axis=-1, keepdims=True)
                norm_sum = norm_part if norm_sum is None else norm_sum + norm_part
            else:
                inbuf[:, at] = following + ((k + 1) / STEPS) * time_embed[:, at]
        if not last:
            inverse = norm_inputs(inbuf[...])

    S("tail")
    norm_row = jnp.transpose(jnp.broadcast_to(norm_sum, (rows, LANES)))[:8]
    half_log = 0.5 * math.log(2.0 * math.pi)
    first_row = lax.broadcasted_iota(jnp.int32, (8, rows), 0) == 0
    stats_out[...] = jnp.where(
        first_row, trace_row, trace_row - 0.5 * norm_row / width - half_log
    )
    for exchanged in all_exchanges + [shards[d] for d in shards]:
        exchanged[4]()
    for d in fetches:
        fetches[d].wait_send()
    S("meanwait")
    z_wait(mean_copies)
    total = jnp.sum(sumbuf[...], axis=0)
    mean_out[...] = jnp.broadcast_to(total / frames - half_log, (8, LANES))
    S(None)


def per_device(
    n,
    m,
    latent,
    probe,
    time_embed,
    gain_attn,
    w_query,
    w_key,
    w_value,
    w_out,
    gain_mlp,
    w_in,
    w_down,
):
    rows, width = latent.shape
    cols = w_query.shape[1]
    hidden = w_in.shape[1]
    part = rows // m
    piece = width // CHUNKS
    pairs = cols // LANES
    frames = rows * n
    vmem = pl.BlockSpec(memory_space=pltpu.VMEM)
    anyspace = pl.BlockSpec(memory_space=pl.ANY)
    dma = pltpu.SemaphoreType.DMA
    phases = 2 * pairs + 2 * CHUNKS
    state, stats, mean = pl.pallas_call(
        functools.partial(flow_kernel, n, m),
        out_shape=(
            jax.ShapeDtypeStruct((rows, width), F32),
            jax.ShapeDtypeStruct((8, rows), F32),
            jax.ShapeDtypeStruct((8, LANES), F32),
        ),
        in_specs=[vmem] * 5 + [anyspace] * 6,
        out_specs=(vmem, vmem, vmem),
        scratch_shapes=[
            pltpu.VMEM((width, 3 * cols), BF16),
            pltpu.VMEM((m, cols, width), BF16),
            pltpu.VMEM((width, hidden), BF16),
            pltpu.VMEM((hidden, width), BF16),
            pltpu.VMEM((2 * rows, width), BF16),
            pltpu.VMEM((2, pairs, rows, LANES), BF16),
            pltpu.VMEM((STEPS, 2, pairs, n, rows, LANES), BF16),
            pltpu.VMEM((STEPS, 2, pairs, n, rows, LANES), BF16),
            pltpu.VMEM((STEPS, 2, pairs, m, rows, LANES), BF16),
            pltpu.VMEM((rows, width), F32),
            pltpu.VMEM((rows, hidden), F32),
            pltpu.VMEM((pairs, 2 * rows, frames), F32),
            pltpu.VMEM((pairs, 2 * rows, LANES), F32),
            pltpu.VMEM((pairs, 2 * rows, LANES), F32),
            pltpu.VMEM((rows, width), F32),
            pltpu.VMEM((rows, hidden), F32),
            pltpu.VMEM((rows, width), F32),
            pltpu.VMEM((STEPS, CHUNKS, m, part, piece), BF16),
            pltpu.VMEM((STEPS, CHUNKS, m, part, piece), BF16),
            pltpu.VMEM((part, width), F32),
            pltpu.VMEM((STEPS, CHUNKS, m, part, piece), BF16),
            pltpu.VMEM((m, 8, rows), F32),
            pltpu.VMEM((n * m, 1, LANES), F32),
            dma((6,)),
            dma((m,)),
            dma((m,)),
            dma((m, 2 * n)),
            dma((m, 2, n)),
            dma((STEPS, 2, pairs, 2 * n)),
            dma((STEPS, 2, pairs, 2, n)),
            dma((STEPS, phases, m)),
            dma((STEPS, phases, m)),
            dma((m,)),
            dma((m,)),
            dma((n * m,)),
            dma((n * m,)),
        ],
        compiler_params=pltpu.CompilerParams(
            collective_id=0, has_side_effects=True, vmem_limit_bytes=60 * 1024 * 1024
        ),
    )(
        latent,
        probe,
        time_embed.reshape(1, width),
        gain_attn.reshape(1, width),
        gain_mlp.reshape(1, width),
        w_query,
        w_key,
        w_value,
        w_out,
        w_in,
        w_down,
    )
    return (state, stats[0], stats[1], mean[0, 0])


def solution(mesh):
    return jax.shard_map(
        functools.partial(per_device, mesh.shape["seq"], mesh.shape["head"]),
        mesh=mesh,
        in_specs=(
            P("seq", None),
            P("seq", None),
            P(),
            P(),
            P(None, "head"),
            P(None, "head"),
            P(None, "head"),
            P("head", None),
            P(),
            P(None, "head"),
            P("head", None),
        ),
        out_specs=(P("seq", None), P("seq"), P("seq"), P()),
        check_vma=False,
    )
```

```python
import functools
import math

import jax
import jax.numpy as jnp
from jax import lax
from jax.experimental import pallas as pl
from jax.experimental.pallas import tpu as pltpu
from jax.sharding import PartitionSpec as P

HEAD_DIM = 64
STEPS = 2
EPSILON = 1e-05
GELU_COEF = 0.044715
ROOT_TWO_PI = math.sqrt(2.0 / math.pi)
LANES = 128
CHUNKS = 2
BF16 = jnp.bfloat16
F32 = jnp.float32


def norm_scale(values):
    return lax.rsqrt(jnp.mean(values * values, axis=-1, keepdims=True) + EPSILON)


def norm_tangent(values, tangent, inverse, norm_gain):
    inner_mean = jnp.mean(values * tangent, axis=-1, keepdims=True)
    cubed = inverse * inverse * inverse
    return ((tangent * inverse - values * (cubed * inner_mean)) * norm_gain).astype(BF16)


def gelu_slope(pre_act):
    square = pre_act * pre_act
    tanh_value = jnp.tanh(ROOT_TWO_PI * pre_act * (1.0 + GELU_COEF * square))
    half = 0.5 * (1.0 + tanh_value)
    slope_value = half + 0.5 * pre_act * (1.0 - tanh_value * tanh_value) * (
        ROOT_TWO_PI * (1.0 + 3.0 * GELU_COEF * square)
    )
    return ((pre_act * half).astype(BF16), slope_value)


def dot(a, b):
    return jnp.dot(a, b, preferred_element_type=F32)


def dot_t(a, b):
    return lax.dot_general(a, b, (((1,), (1,)), ((), ())), preferred_element_type=F32)


def flow_kernel(
    n,
    m,
    latent,
    probe,
    time_embed,
    gain_attn,
    gain_mlp,
    w_query,
    w_key,
    w_value,
    w_out,
    w_in,
    w_down,
    latent_end,
    stats_out,
    mean_out,
    wqkv,
    wout,
    win,
    wdown,
    normed,
    qbuf,
    kvbuf,
    headall,
    inbuf,
    probe_down,
    weightbuf,
    primbuf,
    totalbuf,
    midbuf,
    slopebuf,
    partial,
    rssend,
    passbuf,
    rsrecv,
    state,
    delta,
    tracebuf,
    sumbuf,
    lsem,
    fetchsem,
    shardsem,
    kvsend,
    primrecv,
    tangrecv,
    zsem,
    allsem,
):
    s = lax.axis_index("seq")
    z = lax.axis_index("head")
    rows, width = latent.shape
    part = rows // m
    piece = width // CHUNKS
    cols = w_query.shape[1]
    pairs = cols // LANES
    frames = rows * n
    near = n == 8

    def flip(bit):
        return s + bit - 2 * bit * lax.rem(s // bit, 2)

    def zflip(mask):
        twos = z // 2
        ones = z - 2 * twos
        if mask & 1:
            ones = 1 - ones
        if mask & 2:
            twos = 1 - twos
        return 2 * twos + ones

    def zpeer(d):
        return lax.rem(z + d, m)

    def zfrom(d):
        return lax.rem(z + m - d, m)

    def remote(src, dst, send, recv, target_s, target_z):
        return pltpu.make_async_remote_copy(
            src_ref=src,
            dst_ref=dst,
            send_sem=send,
            recv_sem=recv,
            device_id=(target_s, target_z),
            device_id_type=pl.DeviceIdType.MESH,
        )

    scope = [None]

    def S(name):
        if scope[0] is not None:
            scope[0].__exit__(None, None, None)
        scope[0] = None
        if name is not None:
            scope[0] = jax.named_scope(name)
            scope[0].__enter__()

    S("start")
    loads = [
        pltpu.make_async_copy(w_query, wqkv.at[:, pl.ds(0, cols)], lsem.at[0]),
        pltpu.make_async_copy(w_key, wqkv.at[:, pl.ds(cols, cols)], lsem.at[1]),
        pltpu.make_async_copy(w_value, wqkv.at[:, pl.ds(2 * cols, cols)], lsem.at[2]),
        pltpu.make_async_copy(w_out, wout.at[z], lsem.at[3]),
        pltpu.make_async_copy(w_in, win, lsem.at[4]),
        pltpu.make_async_copy(w_down, wdown, lsem.at[5]),
    ]
    for index in (3, 1, 2, 0, 5, 4):
        loads[index].start()

    barrier = pltpu.get_barrier_semaphore()

    peers = [(s, zpeer(d)) for d in range(1, m)] + [(lax.rem(s + d, n), z) for d in range(1, n)]
    for peer in peers:
        pl.semaphore_signal(barrier, inc=1, device_id=peer, device_id_type=pl.DeviceIdType.MESH)

    own_rows = pl.ds(pl.multiple_of(z * part, part), part)
    direction = probe[...].astype(F32)

    def norm_inputs(values):
        inverse = norm_scale(values)
        normed[:rows, :] = (values * inverse * gain_attn[...]).astype(BF16)
        return inverse

    def norm_inputs_tangent(values, inverse):
        normed[rows:, :] = norm_tangent(
            values, probe[...].astype(F32), inverse, gain_attn[...]
        )

    first_values = latent[...].astype(F32)
    inbuf[...] = first_values
    inverse = norm_inputs(first_values)
    norm_inputs_tangent(first_values, inverse)
    state[...] = latent[own_rows, :].astype(F32)

    S("barrier")
    pl.semaphore_wait(barrier, n + m - 2)

    partner = flip(1)
    xn, yn = flip(2), flip(4)
    dn = yn + 2 - 4 * lax.rem(yn // 2, 2)

    def exchange(view, landing, span, sends, lands, fine):
        count = [0]

        def give(which, slot, target, there, sem):
            remote(
                view(which, slot), landing(which, slot, there), sends, lands(sem), target, z
            ).start()
            count[0] += 1

        def got(sem, number):
            pltpu.make_async_copy(span(number), span(number), lands(sem)).wait()

        sems = (0, 1, 2, 3, 4, 5, 6) if fine else (0, 0, 1, 1, 1, 1, 2)

        def own(which):
            if near:
                over_x = (xn, 2, sems[0 if which == 0 else 3])
                over_y = (yn, 4, sems[2 if which == 0 else 1])
                for hop in (over_x, over_y) if which == 0 else (over_y, over_x):
                    give(which, 0, *hop)
                give(which, 0, partner, 1, sems[6])
            else:
                for d in range(1, n):
                    give(which, 0, lax.rem(s + d, n), n - d, sems[6])

        def relay():
            if near:
                got(sems[0], 1 if fine else 2)
                give(0, 2, yn, 6, sems[4])
                if fine:
                    got(sems[1], 1)
                give(1, 4, xn, 6, sems[5])
                give(0, 2, partner, 3, sems[6])
                give(1, 4, partner, 5, sems[6])

        def rest():
            if near:
                if not fine:
                    got(sems[2], 4)
                for which, slot, sem in ((0, 4, 2), (1, 2, 3), (0, 6, 4), (1, 6, 5)):
                    if fine:
                        got(sems[sem], 1)
                    give(which, slot, partner, slot + 1, sems[6])

        def finish():
            got(sems[6], n if near else 2 * n - 2)

        def drain():
            pltpu.make_async_copy(span(count[0]), span(count[0]), sends).wait()

        return own, relay, rest, finish, drain

    def kv_exchange(k, t, p):
        return exchange(
            lambda which, slot: kvbuf.at[k, t, p, which * n + slot],
            lambda which, slot, there: kvbuf.at[k, t, p, which * n + there],
            lambda number: kvbuf.at[k, t, p, pl.ds(0, number)],
            kvsend.at[k, t, p],
            lambda sem: tangrecv.at[k, p, sem] if t else primrecv.at[k, p, sem],
            t == 0,
        )

    line = m == 4
    inner = jnp.logical_and(z > 0, z < m - 1)
    sources = (1, 2, 3) if line else tuple(range(1, m))

    def zsource(index):
        return zflip(index) if line else zfrom(index)

    def waited(ref, sem):
        pltpu.make_async_copy(ref, ref, sem).wait()

    def z_gather(view, span, sem, own_sems=False):
        def landing(index):
            if own_sems:
                return sem(index)
            return sem(1) if line and index == 2 else sem(2)

        def send(block, target, index):
            remote(view(block), view(block), sem(0), landing(index), s, target).start()

        def start():
            if line:
                send(z, zflip(2), 2)
                send(z, zflip(1), 1)

                @pl.when(inner)
                def _():
                    send(z, zflip(3), 3)
            else:
                for d in range(m - 1, 0, -1):
                    send(z, zpeer(d), d)

        def relay():
            if line:
                waited(span(1), landing(2))

                @pl.when(inner)
                def _():
                    send(zflip(2), zflip(1), 3)

        def finish(index):
            if not (line and index == 2):
                waited(span(1), landing(index))

        def finish_all():
            waited(span(2 if line else m - 1), sem(2))

        def drain():
            if line:

                @pl.when(inner)
                def _():
                    waited(span(4), sem(0))

                @pl.when(jnp.logical_not(inner))
                def _():
                    waited(span(2), sem(0))
            else:
                waited(span(m - 1), sem(0))

        return start, relay, finish, finish_all, drain

    def z_reduce(block, passed, landed, span, sem):
        def send(source, target, slot):
            landing = sem(1) if line and slot == 0 else sem(2)
            remote(source, landed(slot), sem(0), landing, s, target).start()

        def start():
            if line:

                @pl.when(jnp.logical_not(inner))
                def _():
                    send(block(zflip(3)), zflip(1), 0)
                    send(block(zflip(2)), zflip(2), 2)

                @pl.when(inner)
                def _():
                    send(block(zflip(3)), zflip(3), 3)

                send(block(zflip(1)), zflip(1), 1)
            else:
                for d in range(m - 1, 0, -1):
                    send(block(zpeer(d)), zpeer(d), d)

        def relay():
            if line:

                @pl.when(inner)
                def _():
                    waited(span(1), sem(1))
                    both = landed(0)[...].astype(F32) + block(zflip(2))[...].astype(F32)
                    passed[...] = both.astype(BF16)
                    send(passed, zflip(2), 2)

        def finish():
            if line:

                @pl.when(inner)
                def _():
                    waited(span(3), sem(2))

                @pl.when(jnp.logical_not(inner))
                def _():
                    waited(span(2), sem(2))
                    landed(3)[...] = jnp.zeros(landed(3).shape, BF16)
            else:
                waited(span(m - 1), sem(2))

        def drain():
            waited(span(3 if line else m - 1), sem(0))

        return start, relay, finish, drain

    block = cols // n if near else cols
    strip = block // 2
    loads[3].wait()

    def block_at(slot):
        if near:
            return pl.ds(pl.multiple_of(slot * block, block), block)
        return pl.ds(0, cols)

    def strip_at(which, slot):
        return pl.ds(pl.multiple_of(slot * block + which * strip, strip), strip)

    fetch = z_gather(
        lambda j: wout.at[j, block_at(s)],
        lambda number: wout.at[pl.ds(0, number), block_at(0)],
        lambda d: fetchsem.at[d],
        own_sems=True,
    )
    fetch[0]()

    def place(slot):
        where = (s, xn, yn, dn)[slot // 2]
        return where if slot % 2 == 0 else where + 1 - 2 * lax.rem(where, 2)

    def shard_exchange(d):
        return exchange(
            lambda which, slot: wout.at[zsource(d), strip_at(which, place(slot))],
            lambda which, slot, there: wout.at[zsource(d), strip_at(which, place(slot))],
            lambda number: wout.at[0, pl.ds(0, number * strip)],
            shardsem.at[d, 3],
            lambda sem: shardsem.at[d, sem],
            False,
        )

    shards = {d: shard_exchange(d) for d in sources} if near else {}

    def shard_own(d):
        fetch[2](d)
        if near:
            shards[d][0](0)
            shards[d][0](1)

    def shard_do(stage, chosen):
        if near:
            for d in chosen:
                shards[d][stage]()

    gathers = []

    def gather(k, phase, view, span):
        gathers.append(z_gather(view, span, lambda index: zsem.at[k, phase, index]))
        return gathers[-1]

    def spread(ref, pair, targets, at):
        for target_s, target_z in targets:
            remote(
                ref.at[at], ref.at[at], allsem.at[pair], allsem.at[pair + 1], target_s, target_z
            ).start()

    def settle(ref, pair, targets):
        block = ref.at[pl.ds(0, len(targets))]
        waited(block, allsem.at[pair])
        waited(block, allsem.at[pair + 1])

    lane = lax.broadcasted_iota(jnp.int32, (1, LANES), 1)
    first = (lane // HEAD_DIM) == 0
    scale = HEAD_DIM ** (-0.5)

    def project(k, which, t):
        if k == 0 and t == 0:
            loads[which].wait()
        weight = wqkv[:, which * cols : (which + 1) * cols]
        return dot(normed[t * rows : (t + 1) * rows, :], weight).astype(BF16)

    def keep_pairs(which, k, t, value):
        for p in range(pairs):
            kvbuf[k, t, p, which * n] = value[:, p * LANES : (p + 1) * LANES]

    def whole(k, t, p, which):
        return kvbuf[k, t, p, which * n : (which + 1) * n].reshape(frames, LANES)

    def two_heads(value):
        zero = jnp.zeros_like(value)
        return jnp.concatenate(
            [jnp.where(first, value, zero), jnp.where(first, zero, value)], axis=0
        )

    def join_heads(value):
        return jnp.where(first, value[:rows], value[rows:]).astype(BF16)

    def attention(k, p):
        keys = whole(k, 0, p, 0)
        vals = whole(k, 0, p, 1)
        scores = dot_t(two_heads(qbuf[k, 0, p]), keys) * scale
        weights = jnp.exp(scores - jnp.max(scores, axis=-1, keepdims=True))
        total = jnp.sum(weights, axis=-1, keepdims=True)
        weightbuf[p] = weights
        prim = dot(weights.astype(BF16), vals) / total
        primbuf[p] = prim
        totalbuf[p] = jnp.broadcast_to(total, (2 * rows, LANES))
        headall[k, 0, p, z] = join_heads(prim)

    def attention_tangent(k, p):
        both_keys = jnp.concatenate([whole(k, 0, p, 0), whole(k, 1, p, 0)], axis=1)
        vals = whole(k, 0, p, 1)
        val_tang = whole(k, 1, p, 1)
        both = jnp.concatenate([two_heads(qbuf[k, 1, p]), two_heads(qbuf[k, 0, p])], axis=1)
        score_tang = dot_t(both, both_keys) * scale
        weights = weightbuf[p]
        weighted = weights * score_tang
        carried = jnp.sum(weighted, axis=-1, keepdims=True)
        mixed = dot(weighted.astype(BF16), vals) + dot(weights.astype(BF16), val_tang)
        total = totalbuf[p]
        tang = mixed / total - (carried / total) * primbuf[p]
        headall[k, 1, p, z] = join_heads(tang)

    def heads_gather(k, t, p):
        return gather(
            k,
            t * pairs + p,
            lambda j: headall.at[k, t, p, j],
            lambda number: headall.at[k, t, p, pl.ds(0, number)],
        )

    def out_project(k, t):
        heads = [headall[k, t, p, j] for j in range(m) for p in range(pairs)]
        return dot(jnp.concatenate(heads, axis=1), wout[...].reshape(m * cols, width))

    def mlp(k):
        attn = out_project(k, 0)
        mid = inbuf[...] + attn
        midbuf[...] = mid
        scaled = (mid * norm_scale(mid) * gain_mlp[...]).astype(BF16)
        if k == 0:
            loads[4].wait()
        act, slope = gelu_slope(dot(scaled, win[...]))
        slopebuf[...] = slope
        for c in range(CHUNKS):
            at = slice(c * piece, (c + 1) * piece)
            terms = dot(act, wdown[:, at])
            rssend[k, c] = terms.astype(BF16).reshape(m, part, piece)
            reduces[k][c][0]()
            partial[:, at] = attn[:, at] + terms

    def mlp_tangent(k):
        attn_tang = out_project(k, 1)
        probing = probe[...].astype(F32)
        mid = midbuf[...]
        tangent = norm_tangent(mid, probing + attn_tang, norm_scale(mid), gain_mlp[...])
        act_tang = (slopebuf[...] * dot(tangent, win[...])).astype(BF16)
        return jnp.sum(probing * attn_tang, axis=-1, keepdims=True) / m + jnp.sum(
            act_tang.astype(F32) * probe_down[...], axis=-1, keepdims=True
        )

    def reduce(k, c):
        phase = 2 * pairs + CHUNKS + c
        return z_reduce(
            lambda j: rssend.at[k, c, j],
            passbuf.at[k, c],
            lambda d: rsrecv.at[k, c, d],
            lambda number: rsrecv.at[k, c, pl.ds(0, number)],
            lambda index: zsem.at[k, phase, index],
        )

    reduces = [[reduce(k, c) for c in range(CHUNKS)] for k in range(STEPS)]
    prims = [[kv_exchange(k, 0, p) for p in range(pairs)] for k in range(STEPS)]
    tangs = [[kv_exchange(k, 1, p) for p in range(pairs)] for k in range(STEPS)]
    heads = [[heads_gather(k, 0, p) for p in range(pairs)] for k in range(STEPS)]
    tangent_heads = [[heads_gather(k, 1, p) for p in range(pairs)] for k in range(STEPS)]

    def delta_gather(k, c):
        return gather(
            k,
            2 * pairs + c,
            lambda j: delta.at[k, c, j],
            lambda number: delta.at[k, c, pl.ds(0, number)],
        )

    deltas = [[delta_gather(k, c) for c in range(CHUNKS)] for k in range(STEPS)]
    trace = None

    for k in range(STEPS):
        last = k == STEPS - 1

        S(f"projk_{k}")
        keep_pairs(0, k, 0, project(k, 1, 0))
        prims[k][0][0](0)
        S(f"projv_{k}")
        keep_pairs(1, k, 0, project(k, 2, 0))
        prims[k][0][0](1)
        for p in range(1, pairs):
            prims[k][p][0](0)
            prims[k][p][0](1)
        if k > 0:
            S(f"normt_{k}")
            for p in range(pairs):
                tangent_heads[k - 1][p][0]()
            norm_inputs_tangent(inbuf[...], inverse)
        S(f"projq_{k}")
        query = project(k, 0, 0)
        for p in range(pairs):
            qbuf[k, 0, p] = query[:, p * LANES : (p + 1) * LANES]
        S(f"projt_{k}")
        keep_pairs(0, k, 1, project(k, 1, 1))
        keep_pairs(1, k, 1, project(k, 2, 1))
        query = project(k, 0, 1)
        for p in range(pairs):
            qbuf[k, 1, p] = query[:, p * LANES : (p + 1) * LANES]
        S(f"relay0_{k}")
        prims[k][0][1]()
        if k == 0:
            S(f"fetchrelay_{k}")
            fetch[1]()
            shard_own(sources[0])
        S(f"relay1_{k}")
        for p in range(1, pairs):
            prims[k][p][1]()
        if k == 0:
            S(f"shard0_{k}")
            shard_own(sources[1])
        else:
            for p in range(pairs):
                tangs[k][p][0](0)
                tangs[k][p][0](1)
        S(f"rest0_{k}")
        prims[k][0][2]()
        if k > 0:
            S(f"trelayz_{k-1}")
            for p in range(pairs):
                tangent_heads[k - 1][p][1]()
        S(f"finish0_{k}")
        prims[k][0][3]()
        S(f"attn_{k}_0")
        attention(k, 0)
        heads[k][0][0]()
        if k == 0:
            S(f"shard1_{k}")
            shard_own(sources[2])
            shard_do(1, sources[:2])
        else:
            S(f"trelay_{k}_0")
            tangs[k][0][1]()
        for p in range(1, pairs):
            S(f"rest1_{k}")
            prims[k][p][2]()
            prims[k][p][3]()
            S(f"attn_{k}_{p}")
            attention(k, p)
            heads[k][p][0]()

        if k == 0:
            S("shard_rest")
            shard_do(2, sources[:2])
            shard_do(1, sources[2:])
            for p in range(pairs):
                tangs[k][p][0](0)
                tangs[k][p][0](1)
            S("probe_down")
            loads[5].wait()
            probe_down[...] = dot_t(probe[...], wdown[...])
            S("headrelay_0")
            for p in range(pairs):
                heads[k][p][1]()
            S("shard_finish")
            shard_do(3, sources[:2])
            shard_do(2, sources[2:])
            S("shard_finish2")
            shard_do(3, sources[2:])
        else:
            S(f"trelay_{k}_1")
            for p in range(1, pairs):
                tangs[k][p][1]()
            S(f"trest_{k}_0")
            tangs[k][0][2]()
            S(f"theads_{k-1}")
            for p in range(pairs):
                tangent_heads[k - 1][p][3]()
            S(f"tmlp_{k-1}")
            grown = mlp_tangent(k - 1)
            trace = grown if trace is None else trace + grown
            S(f"headrelay_{k}_0")
            heads[k][0][1]()
            S(f"tfinish_{k}_0")
            tangs[k][0][3]()
            S(f"tattn_{k}_0")
            attention_tangent(k, 0)
            tangent_heads[k][0][0]()
            for p in range(1, pairs):
                S(f"headrelay_{k}_{p}")
                heads[k][p][1]()
                S(f"tfinish_{k}_{p}")
                tangs[k][p][2]()
                tangs[k][p][3]()
                S(f"tattn_{k}_{p}")
                attention_tangent(k, p)
                if last:
                    tangent_heads[k][p][0]()

        S(f"heads_{k}")
        for p in range(pairs):
            heads[k][p][3]()
        S(f"mlp_{k}")
        mlp(k)

        if k == 0:
            for p in range(pairs):
                S(f"trelay_{k}_{p}")
                tangs[k][p][1]()
        for c in range(CHUNKS):
            S(f"rsrelay_{k}_{c}")
            reduces[k][c][1]()
        if last:
            S(f"threlay_{k}")
            for p in range(pairs):
                tangent_heads[k][p][1]()
            S(f"theads_{k}")
            for p in range(pairs):
                tangent_heads[k][p][3]()
            S(f"tmlp_{k}")
            trace = trace + mlp_tangent(k)
            column = trace / (STEPS * width)
            trace_sum = jnp.sum(column, axis=0, keepdims=True)
            tracebuf[z] = jnp.transpose(jnp.broadcast_to(column, (rows, LANES)))[:8, :]
            ring = [(s, zpeer(d)) for d in range(1, m)]
            spread(tracebuf, 0, ring, z)

        squares = jnp.zeros((1, 1), F32)
        for c in range(CHUNKS):
            at = slice(c * piece, (c + 1) * piece)
            S(f"rswait_{k}_{c}")
            reduces[k][c][2]()
            S(f"field_{k}_{c}")
            field = partial[own_rows, at]
            for d in sources:
                field = field + rsrecv[k, c, d].astype(F32)
            new_state = state[:, at] + field / STEPS
            state[:, at] = new_state
            delta[k, c, z] = (new_state - latent[own_rows, at].astype(F32)).astype(BF16)
            if last:
                by_row = jnp.sum(new_state * new_state, axis=-1, keepdims=True)
                squares = squares + jnp.sum(by_row, axis=0, keepdims=True)
                if c == CHUNKS - 1:
                    sumbuf[s * m + z] = jnp.broadcast_to(
                        trace_sum - 0.5 * squares / width, (1, LANES)
                    )
                    others = [
                        (lax.rem(s + a, n), lax.rem(z + b, m))
                        for a in range(n)
                        for b in range(m)
                        if a or b
                    ]
                    spread(sumbuf, 2, others, s * m + z)
            deltas[k][c][0]()
        if not last:
            for p in range(pairs):
                S(f"trest_{k}_{p}")
                tangs[k][p][2]()
            S(f"deltarelay_{k}")
            for c in range(CHUNKS):
                deltas[k][c][1]()
            for p in range(pairs):
                S(f"tfinish_{k}_{p}")
                tangs[k][p][3]()
                S(f"tattn_{k}_{p}")
                attention_tangent(k, p)
        else:
            S("deltarelay_1_0")
            deltas[k][0][1]()
            S("deltarelay_1_1")
            for c in range(1, CHUNKS):
                deltas[k][c][1]()
            settle(tracebuf, 0, ring)
            trace_row = jnp.sum(tracebuf[...], axis=0)

        norm_sum = None
        for c in range(CHUNKS):
            at = slice(c * piece, (c + 1) * piece)
            S(f"deltawait_{k}_{c}")
            deltas[k][c][3]()
            S(f"norm_{k}_{c}")
            following = latent[:, at].astype(F32) + delta[k, c].reshape(rows, piece).astype(F32)
            if last:
                latent_end[:, at] = following
                norm_part = jnp.sum(following * following, axis=-1, keepdims=True)
                norm_sum = norm_part if norm_sum is None else norm_sum + norm_part
            else:
                inbuf[:, at] = following + ((k + 1) / STEPS) * time_embed[:, at]
        if not last:
            inverse = norm_inputs(inbuf[...])

    S("tail")
    norm_row = jnp.transpose(jnp.broadcast_to(norm_sum, (rows, LANES)))[:8]
    half_log = 0.5 * math.log(2.0 * math.pi)
    first_row = lax.broadcasted_iota(jnp.int32, (8, rows), 0) == 0
    stats_out[...] = jnp.where(
        first_row, trace_row, trace_row - 0.5 * norm_row / width - half_log
    )
    for k in range(STEPS):
        for exchanged in prims[k] + tangs[k]:
            exchanged[4]()
        for reduced in reduces[k]:
            reduced[3]()
    for d in shards:
        shards[d][4]()
    for gathered in gathers + [fetch]:
        gathered[4]()
    S("meanwait")
    settle(sumbuf, 2, others)
    total = jnp.sum(sumbuf[...], axis=0)
    mean_out[...] = jnp.broadcast_to(total / frames - half_log, (8, LANES))
    S(None)


def finish_kernel(state, stats, mean, latent_end, trace, logp, total):
    latent_end[...] = state[...]
    trace[...] = stats[0:1, :]
    logp[...] = stats[1:2, :]
    total[...] = mean[0:1, 0:1]


def per_device(
    n,
    m,
    latent,
    probe,
    time_embed,
    gain_attn,
    w_query,
    w_key,
    w_value,
    w_out,
    gain_mlp,
    w_in,
    w_down,
):
    rows, width = latent.shape
    cols = w_query.shape[1]
    hidden = w_in.shape[1]
    part = rows // m
    piece = width // CHUNKS
    pairs = cols // LANES
    frames = rows * n
    vmem = pl.BlockSpec(memory_space=pltpu.VMEM)
    anyspace = pl.BlockSpec(memory_space=pl.ANY)
    dma = pltpu.SemaphoreType.DMA
    phases = 2 * pairs + 2 * CHUNKS
    state, stats, mean = pl.pallas_call(
        functools.partial(flow_kernel, n, m),
        out_shape=(
            jax.ShapeDtypeStruct((rows, width), F32),
            jax.ShapeDtypeStruct((8, rows), F32),
            jax.ShapeDtypeStruct((8, LANES), F32),
        ),
        in_specs=[vmem] * 5 + [anyspace] * 6,
        out_specs=(vmem, vmem, vmem),
        scratch_shapes=[
            pltpu.VMEM((width, 3 * cols), BF16),
            pltpu.VMEM((m, cols, width), BF16),
            pltpu.VMEM((width, hidden), BF16),
            pltpu.VMEM((hidden, width), BF16),
            pltpu.VMEM((2 * rows, width), BF16),
            pltpu.VMEM((STEPS, 2, pairs, rows, LANES), BF16),
            pltpu.VMEM((STEPS, 2, pairs, 2 * n, rows, LANES), BF16),
            pltpu.VMEM((STEPS, 2, pairs, m, rows, LANES), BF16),
            pltpu.VMEM((rows, width), F32),
            pltpu.VMEM((rows, hidden), F32),
            pltpu.VMEM((pairs, 2 * rows, frames), F32),
            pltpu.VMEM((pairs, 2 * rows, LANES), F32),
            pltpu.VMEM((pairs, 2 * rows, LANES), F32),
            pltpu.VMEM((rows, width), F32),
            pltpu.VMEM((rows, hidden), F32),
            pltpu.VMEM((rows, width), F32),
            pltpu.VMEM((STEPS, CHUNKS, m, part, piece), BF16),
            pltpu.VMEM((STEPS, CHUNKS, part, piece), BF16),
            pltpu.VMEM((STEPS, CHUNKS, m, part, piece), BF16),
            pltpu.VMEM((part, width), F32),
            pltpu.VMEM((STEPS, CHUNKS, m, part, piece), BF16),
            pltpu.VMEM((m, 8, rows), F32),
            pltpu.VMEM((n * m, 1, LANES), F32),
            dma((6,)),
            dma((m,)),
            dma((m, 4)),
            dma((STEPS, 2, pairs)),
            dma((STEPS, pairs, 7)),
            dma((STEPS, pairs, 3)),
            dma((STEPS, phases, 3)),
            dma((4,)),
        ],
        compiler_params=pltpu.CompilerParams(
            collective_id=0,
            has_side_effects=True,
            vmem_limit_bytes=60 * 1024 * 1024,
        ),
    )(
        latent,
        probe,
        time_embed.reshape(1, width),
        gain_attn.reshape(1, width),
        gain_mlp.reshape(1, width),
        w_query,
        w_key,
        w_value,
        w_out,
        w_in,
        w_down,
    )
    latent_end, trace, logp, total = pl.pallas_call(
        finish_kernel,
        out_shape=(
            jax.ShapeDtypeStruct((rows, width), F32),
            jax.ShapeDtypeStruct((1, rows), F32),
            jax.ShapeDtypeStruct((1, rows), F32),
            jax.ShapeDtypeStruct((1, 1), F32),
        ),
        in_specs=[vmem] * 3,
        out_specs=(vmem,) * 4,
    )(state, stats, mean)
    return (latent_end, trace.reshape(rows), logp.reshape(rows), total.reshape(()))


def solution(mesh):
    return jax.shard_map(
        functools.partial(per_device, mesh.shape["seq"], mesh.shape["head"]),
        mesh=mesh,
        in_specs=(
            P("seq", None),
            P("seq", None),
            P(),
            P(),
            P(None, "head"),
            P(None, "head"),
            P(None, "head"),
            P("head", None),
            P(),
            P(None, "head"),
            P("head", None),
        ),
        out_specs=(P("seq", None), P("seq"), P("seq"), P()),
        check_vma=False,
    )
```
